256 devices in a mesh: rep: 2 (over y), seq: 128 (over z, x, core).
Axes of the slice: x: 4, y: 2, z: 16, core: 2. Of those that a mesh axis runs over, the one named last changes fastest.
The devices are a block of a 4x16x16 slice.
Arguments:
- latents: bfloat16 [16, 196608], P(None, ('rep', 'seq')), parts along dimension 1, may hold values from -6 to 6
- layout: int32 [256, 768], P('rep'), parts along dimension 0, may hold values from 0 to 98303, as said below
- assign: int32 [16], P('rep'), parts along dimension 0, may hold values from 0 to 7, as said below
- counts: int32 [16], P('rep'), parts along dimension 0, may hold values from 1 to 3
- latent_cache: bfloat16 [2, 1024, 1024], P(None, ('rep', 'seq')), parts along dimension 1, may hold values from -6 to 6
- feature_cache: bfloat16 [2, 1024, 64, 384], P(None, ('rep', 'seq')), parts along dimension 1, may hold values from -4 to 4
- first_weight: bfloat16 [3, 3, 3, 16, 384], replicated, may hold values from -0.3125 to 0.3125
- first_bias: float32 [384], replicated, may hold values from -3 to 3
- norm_gain: float32 [384], replicated, may hold values from 0.25 to 1.75
- second_weight: bfloat16 [3, 3, 3, 384, 192], replicated, may hold values from -0.0625 to 0.0625
- second_bias: float32 [192], replicated, may hold values from -3 to 3
Outputs:
- decoded_frames: bfloat16 [3, 2048, 128, 192], P(None, ('rep', 'seq')), parts along dimension 1
- latent_cache_next: bfloat16 [2, 1024, 1024], P(None, ('rep', 'seq')), parts along dimension 1
- feature_cache_next: bfloat16 [2, 1024, 64, 384], P(None, ('rep', 'seq')), parts along dimension 1
The draws below stay inside these ranges and needn't reach their ends.
There are 2 independent parts, one for each index of `rep`. The reference program is written for one: setup_inputs(seed, part) draws one part's arguments, and reference() takes and returns one part's arrays. A program takes and returns all parts, laid end to end along the dimension named above; an argument that names none is the same for every part. Nothing has to cross between parts.
Inputs may be any that keep to these rules, and one draw needn't show every extreme that they name: assign is a permutation of 0 to 7. layout is a permutation of 0 to 98303. Call the cells of request assign[g], rows k * 4 to (k + 1) * 4 - 1, all frames and columns, the tile of seq index (g * 16 + k - 8) mod 128; every row of layout holds exactly 6 cells of every tile.
All inputs are finite; a program needn't handle non-finite values.
Results may differ from the reference program's by a relative error of at most 0.0034.
Values may be sent and summed in bfloat16 or wider, within the bound.
No kernel may reach another device: no remote copies, remote signals or barrier semaphores. Data moves between devices by JAX's collectives and lax.ppermute only.
A program may use at most 128 MiB of HBM per device.

```python
import jax
import jax.numpy as jnp
from jax import lax

LAT_CH = 16
MID_CH = 384
OUT_CH = 192
REQS = 8
FMAX = 3
ROWS_DEV = 4
W = 64
GROUP = 16
SHIFT = 8
HEIGHT = 64
CELLS = 768
PEER = 6
TOTAL_CELLS = 98304
ROWS_ALL = 512
N_SEQ = 128


def pairing(key):
    return jax.random.permutation(jax.random.fold_in(key, 11), REQS).astype(jnp.int32)


def one_permutation(subkey):
    return jax.random.permutation(subkey, CELLS).astype(jnp.int32)


def draw_assign(key, part):
    return pairing(key)


def draw_layout(key, part):
    assign = pairing(key)
    spread_keys = jax.random.split(jax.random.fold_in(key, 23), N_SEQ)
    within = jax.vmap(one_permutation)(spread_keys)
    numbers = jnp.arange(N_SEQ, dtype=jnp.int32)[:, None] * CELLS + within
    numbers = jnp.transpose(numbers.reshape(N_SEQ, N_SEQ, PEER), (1, 0, 2)).reshape(N_SEQ, CELLS)
    slot_keys = jax.random.split(jax.random.fold_in(key, 37), N_SEQ)
    mixing = jax.vmap(one_permutation)(slot_keys)
    numbers = jnp.take_along_axis(numbers, mixing, axis=1)
    target = numbers // CELLS
    inside = numbers % CELLS
    frame_index = inside // (ROWS_DEV * W)
    tile_row = inside // W % ROWS_DEV
    column = inside % W
    place = (target + SHIFT) % N_SEQ
    group_index = place // GROUP
    position = place % GROUP
    request = jnp.take(assign, group_index)
    image_row = position * ROWS_DEV + tile_row
    return (((request * FMAX + frame_index) * HEIGHT + image_row) * W + column).astype(jnp.int32)


def plant(entries, key, smallest, top_value):
    spot = [jax.random.randint(jax.random.fold_in(key, axis), (), 0, length) for axis, length in enumerate(entries.shape)]
    longest = entries.shape.index(max(entries.shape))
    neighbour = spot[:longest] + [(spot[longest] + 1) % entries.shape[longest]] + spot[longest + 1:]
    return entries.at[tuple(spot)].set(smallest).at[tuple(neighbour)].set(top_value)


def levels(rng, extent, cuts, low, largest):
    factor_of = 1.0
    for axis_at, blocks in cuts:
        draws = jax.random.uniform(jax.random.fold_in(jax.random.fold_in(rng, 6), axis_at), (blocks,), jnp.float32, low / len(cuts), largest / len(cuts))
        factor_of = factor_of * jnp.repeat(jnp.exp(draws), extent[axis_at] // blocks).reshape((-1,) + (1,) * (len(extent) - 1 - axis_at))
    return factor_of


def scatter_about(key, shape, deviation, bound, pieces=(), kind=jnp.bfloat16):
    values = jax.random.normal(key, shape, jnp.float32) * deviation
    if len(pieces) > 0:
        values = levels(key, shape, pieces, -0.22, 0.18) * values
    return jnp.clip(values, min=-bound, max=bound).astype(kind)


def setup_inputs(seed: int = 0, part: int = 0) -> dict:
    key_of = jax.random.split(jax.random.key(seed), 12)
    part_keys = jax.random.split(jax.random.fold_in(key_of[11], part), 12)
    return {
        "latents": scatter_about(part_keys[0], (LAT_CH, TOTAL_CELLS), 1.0, 6.0, ((1, 128),)),
        "layout": draw_layout(jax.random.fold_in(jax.random.fold_in(key_of[11], part), 71), part),
        "assign": draw_assign(jax.random.fold_in(jax.random.fold_in(key_of[11], part), 71), part),
        "counts": plant(jax.random.randint(part_keys[3], (REQS,), 1, FMAX + 1), jax.random.fold_in(part_keys[3], 1), 1, FMAX).astype(jnp.int32),
        "latent_cache": scatter_about(part_keys[4], (2, ROWS_ALL, W * LAT_CH), 1.0, 6.0, ((1, 128),)),
        "feature_cache": scatter_about(part_keys[5], (2, ROWS_ALL, W, MID_CH), 0.6, 4.0, ((1, 128),)),
        "first_weight": scatter_about(key_of[6], (3, 3, 3, LAT_CH, MID_CH), (27 * LAT_CH) ** -0.5, 0.3125),
        "first_bias": scatter_about(key_of[7], (MID_CH,), 0.5, 3.0, (), jnp.float32),
        "norm_gain": jnp.clip(1.0 + 0.15 * jax.random.normal(key_of[8], (MID_CH,), jnp.float32), 0.25, 1.75),
        "second_weight": scatter_about(key_of[9], (3, 3, 3, MID_CH, OUT_CH), (27 * MID_CH) ** -0.5, 0.0625),
        "second_bias": scatter_about(key_of[10], (OUT_CH,), 0.5, 3.0, (), jnp.float32),
    }


def causal_conv(values, weight, offset):
    result = lax.conv_general_dilated(values[None], weight, (1, 1, 1), ((0, 0), (1, 1), (1, 1)), dimension_numbers=('NDHWC', 'DHWIO', 'NDHWC'), preferred_element_type=jnp.float32)
    return result[0] + offset

def activate(linear, norm_gain):
    inverse = lax.rsqrt(lax.optimization_barrier(jnp.mean(linear * linear, axis=-1, keepdims=True)) + 1e-06)
    return jax.nn.silu(linear * inverse * norm_gain).astype(jnp.bfloat16)

def reference(latents, layout, assign, counts, latent_cache, feature_cache, first_weight, first_bias, norm_gain, second_weight, second_bias):
    positions = jnp.argsort(layout.reshape(-1)).astype(jnp.int32)
    ordered = jnp.take(latents, positions, axis=1).reshape(LAT_CH, REQS, FMAX, HEIGHT, W)
    ordered = jnp.transpose(ordered, (1, 2, 3, 4, 0))
    latent_prev = jnp.roll(latent_cache, SHIFT * ROWS_DEV, axis=1).reshape(2, REQS, HEIGHT, W, LAT_CH)
    feature_prev = jnp.roll(feature_cache, SHIFT * ROWS_DEV, axis=1).reshape(2, REQS, HEIGHT, W, MID_CH)
    frame_index = jnp.arange(FMAX, dtype=jnp.int32)[:, None, None, None]
    decoded_list = []
    latent_list = []
    feature_list = []
    for group_index in range(REQS):
        request = assign[group_index].astype(jnp.int32)
        live_frames = counts[request].astype(jnp.int32)
        window = lax.dynamic_index_in_dim(ordered, request, 0, keepdims=False)
        first_input = jnp.concatenate([latent_prev[:, group_index], window], axis=0)
        features = activate(causal_conv(first_input, first_weight, first_bias), norm_gain)
        second_input = jnp.concatenate([feature_prev[:, group_index], features], axis=0)
        doubled = jnp.repeat(jnp.repeat(second_input, 2, axis=1), 2, axis=2)
        decoded = causal_conv(doubled, second_weight, second_bias)
        decoded = jnp.where(frame_index < live_frames, decoded, 0.0).astype(jnp.bfloat16)
        decoded_list.append(decoded)
        latent_list.append(lax.dynamic_slice_in_dim(first_input, live_frames, 2, 0))
        feature_list.append(lax.dynamic_slice_in_dim(second_input, live_frames, 2, 0))
    decoded_frames = jnp.roll(jnp.concatenate(decoded_list, axis=1), -2 * SHIFT * ROWS_DEV, axis=1)
    latent_cache_next = jnp.roll(jnp.concatenate(latent_list, axis=1), -SHIFT * ROWS_DEV, axis=1).reshape(2, ROWS_ALL, W * LAT_CH)
    feature_cache_next = jnp.roll(jnp.concatenate(feature_list, axis=1), -SHIFT * ROWS_DEV, axis=1)
    return (decoded_frames, latent_cache_next, feature_cache_next)
```

```python
import jax
import jax.numpy as jnp
from jax import lax
from jax.experimental import pallas as pl
from jax.experimental.pallas import tpu as pltpu
from jax.sharding import PartitionSpec as P

LAT_CH = 16
MID_CH = 384
OUT_CH = 192
REQS = 8
FMAX = 3
ROWS_DEV = 4
W = 64
LANES = 128
HALO = 2
WIN_ROWS = ROWS_DEV + 2 * HALO
MID_ROWS = ROWS_DEV + 2
FX = FMAX * W
TILES = 3
BF16 = jnp.bfloat16
F32 = jnp.float32
I32 = jnp.int32
VMEM = pl.BlockSpec(memory_space=pltpu.VMEM)
SMEM = pl.BlockSpec(memory_space=pltpu.SMEM)
ANY = pl.BlockSpec(memory_space=pl.ANY)


def iota(shape, dim):
    return lax.broadcasted_iota(I32, shape, dim)


def dot(a, b, dims=((1,), (0,))):
    return lax.dot_general(a, b, (dims, ((), ())), preferred_element_type=F32)


NT = ((1,), (1,))


def cell_parts(numbers, assign_ref, devices):
    per_group = devices // REQS
    w_bits = W.bit_length() - 1
    height = ROWS_DEV * per_group
    h_bits = height.bit_length() - 1
    column = numbers & (W - 1)
    image_row = (numbers >> w_bits) & (height - 1)
    frames = numbers >> (w_bits + h_bits)
    request = jnp.zeros_like(frames)
    for r in range(1, REQS):
        request = request + (frames >= r * FMAX).astype(I32)
    frame = frames - request * FMAX
    group = jnp.zeros_like(frames)
    for g in range(1, REQS):
        group = jnp.where(request == assign_ref[g], g, group)
    place = group * per_group + image_row // ROWS_DEV
    target = (place - per_group // 2 + devices) & (devices - 1)
    return target, frame, image_row & (ROWS_DEV - 1), column


def earlier(length):
    return (iota((length, length), 0) < iota((length, length), 1)).astype(F32).astype(BF16)


def send_kernel(layout_ref, latents_ref, assign_ref, features_ref, out_ref, last_ref, first_ref, sems):
    devices, slots = layout_ref.shape
    per_peer = slots // devices
    me = lax.axis_index("seq")
    copies = [
        pltpu.make_async_copy(features_ref.at[:, ROWS_DEV - 1], last_ref, sems.at[0]),
        pltpu.make_async_copy(features_ref.at[:, 0], first_ref, sems.at[1]),
    ]
    for copy in copies:
        copy.start()
    base = pl.multiple_of(me // 8 * 8, 8)
    rows = layout_ref[pl.ds(base, 8), :]
    own = jnp.sum(jnp.where(iota(rows.shape, 0) == me - base, rows, 0), axis=0, keepdims=True)
    target = cell_parts(own, assign_ref, devices)[0]
    member = (iota((devices, slots), 0) == target).astype(F32)
    rank = dot(member.astype(BF16), earlier(slots))
    latents = latents_ref[...]
    out = jnp.zeros((devices, LANES), F32)
    for k in range(per_peer):
        picked = jnp.where(rank == float(k), member, 0.0).astype(BF16)
        cells = dot(picked, latents, NT).astype(BF16)
        spot = (iota((LAT_CH, LANES), 1) == iota((LAT_CH, LANES), 0) + k * LAT_CH).astype(F32)
        out = out + dot(cells, spot.astype(BF16))
    out_ref[:, 0:LANES] = pltpu.roll(out, 1, 0).astype(BF16)
    out_ref[:, LANES : 2 * LANES] = out.astype(BF16)
    out_ref[:, 2 * LANES : 3 * LANES] = pltpu.roll(out, devices - 1, 0).astype(BF16)
    for copy in copies:
        copy.wait()


def table_kernel(layout_ref, assign_ref, cache_ref, before_ref, after_ref, hot_ref, code_ref, cached_ref, spread):
    devices, slots = layout_ref.shape
    per_group = devices // REQS
    per_peer = slots // devices
    me = lax.axis_index("seq")
    place = (me + per_group // 2) & (devices - 1)
    position = place & (per_group - 1)
    target, frame, row, column = cell_parts(layout_ref[...], assign_ref, devices)
    order = earlier(slots)
    codes = jnp.zeros((devices, LANES), F32)
    fx = frame * W + column
    lane = iota((devices, LANES), 1)
    for j in range(TILES):
        tile = (me + j - 1 + devices) & (devices - 1)
        hit = target == tile
        rank = dot(hit.astype(F32).astype(BF16), order)
        code = ((row + ROWS_DEV * j) * 256 + fx).astype(F32)
        if j == 0:
            code = jnp.where(position == 0, 0.0, code)
        if j == TILES - 1:
            code = jnp.where(position == per_group - 1, 0.0, code)
        code = jnp.where(hit, code, 0.0)
        for k in range(per_peer):
            one = jnp.sum(jnp.where(rank == float(k), code, 0.0), axis=1, keepdims=True)
            codes = jnp.where(lane == j * per_peer + k, one, codes)
    code_ref[...] = codes
    across = jnp.transpose(codes).astype(I32) & 255
    for jk in range(TILES * per_peer):
        hot = (iota((FX, devices), 0) == across[jk : jk + 1, :]).astype(F32)
        hot_ref[:, jk * devices : (jk + 1) * devices] = hot.astype(BF16)
    width = W * LAT_CH
    keep = iota((W, width), 1) // LAT_CH == iota((W, width), 0)
    repeat = ((iota((width, LANES), 0) & (LAT_CH - 1)) == (iota((width, LANES), 1) & (LAT_CH - 1))).astype(F32).astype(BF16)
    lane = iota((W, LANES), 1) // LAT_CH
    for f in range(2):
        for y in range(WIN_ROWS):
            if y < HALO:
                line = before_ref[f, y + ROWS_DEV - HALO : y + ROWS_DEV - HALO + 1, :].astype(F32)
                line = jnp.where(position == 0, 0.0, line)
            elif y < HALO + ROWS_DEV:
                line = cache_ref[f, y - HALO : y - HALO + 1, :].astype(F32)
            else:
                line = after_ref[f, y - HALO - ROWS_DEV : y - HALO - ROWS_DEV + 1, :].astype(F32)
                line = jnp.where(position == per_group - 1, 0.0, line)
            spread[y * W : (y + 1) * W, :] = jnp.where(keep, line, 0.0).astype(BF16)
        wide = dot(spread[...], repeat)
        total = jnp.zeros((W, LANES), F32)
        for y in range(WIN_ROWS):
            total = jnp.where(lane == y, wide[y * W : (y + 1) * W, :], total)
        cached_ref[f * W : (f + 1) * W, :] = total.astype(BF16)


def weight_kernel(weight_ref, out_ref):
    taps = [[weight_ref[0, b, e].astype(F32) for e in range(3)] for b in range(3)]
    for a, i, rows in ((0, 0, (0,)), (0, 1, (1, 2)), (1, 0, (0, 1)), (1, 1, (2,))):
        line = [sum(taps[b][e] for b in rows[1:]) + taps[rows[0]][e] if len(rows) > 1 else taps[rows[0]][e] for e in range(3)]
        parts = (line[1] + line[2], line[0] + line[1], line[0], line[2])
        for g, part in enumerate(parts):
            out_ref[a, g * OUT_CH : (g + 1) * OUT_CH, i * MID_CH : (i + 1) * MID_CH] = part.astype(BF16)


def shifted(values, step, columns):
    if step == 1:
        return values
    rows = values.shape[0]
    x = iota(values.shape, 0) & (columns - 1)
    if step == 0:
        return jnp.where(x == 0, 0.0, pltpu.roll(values, 1, 0))
    return jnp.where(x == columns - 1, 0.0, pltpu.roll(values, rows - 1, 0))


def decode_kernel(
    incoming_ref,
    hot_ref,
    code_ref,
    cached_ref,
    assign_ref,
    counts_ref,
    first_weight_ref,
    first_bias_ref,
    gain_ref,
    second_bias_ref,
    features_ref,
    before_ref,
    after_ref,
    weight_ref,
    out_ref,
    latent_ref,
    next_ref,
    weight,
    second,
    padded,
    cells,
    window,
    decoded,
    sems,
    out_sems,
):
    devices = lax.axis_size("seq")
    per_group = devices // REQS
    me = lax.axis_index("seq")
    place = (me + per_group // 2) & (devices - 1)
    position = place & (per_group - 1)
    live = counts_ref[assign_ref[place // per_group]]
    copies = [
        pltpu.make_async_copy(features_ref, second.at[0:2, 1 : 1 + ROWS_DEV], sems.at[0]),
        pltpu.make_async_copy(before_ref, second.at[0:2, 0], sems.at[1]),
        pltpu.make_async_copy(after_ref, second.at[0:2, MID_ROWS - 1], sems.at[2]),
        pltpu.make_async_copy(weight_ref, weight, sems.at[3]),
    ]
    for copy in copies:
        copy.start()

    margin = (WIN_ROWS - 3) * LAT_CH
    for a in range(3):
        for e in range(3):
            padded[a * 3 + e, 0:margin, :] = jnp.zeros((margin, MID_CH), BF16)
            padded[a * 3 + e, margin + 3 * LAT_CH :, :] = jnp.zeros((margin, MID_CH), BF16)
            for b in range(3):
                padded[a * 3 + e, margin + b * LAT_CH : margin + (b + 1) * LAT_CH, :] = first_weight_ref[a, b, e]

    pairs = hot_ref.shape[1] // devices
    per_peer = pairs // TILES
    wide = per_peer * LANES
    source = iota((LANES, wide), 1)
    expand = (iota((LANES, wide), 0) == source // LANES * LAT_CH + (source & (LAT_CH - 1))).astype(F32).astype(BF16)
    codes = code_ref[...].astype(I32) >> 8
    lane = iota((devices, LANES), 1) // LAT_CH + HALO
    for j in range(TILES):
        spread = dot(incoming_ref[:, j * LANES : (j + 1) * LANES], expand)
        for k in range(per_peer):
            jk = j * per_peer + k
            part = jnp.where(lane == codes[:, jk : jk + 1], spread[:, k * LANES : (k + 1) * LANES], 0.0)
            cells[jk * devices : (jk + 1) * devices, :] = part.astype(BF16)
    arranged = dot(hot_ref[...], cells[...])
    frames = jnp.concatenate([cached_ref[...].astype(F32), arranged], axis=0)
    for e in range(3):
        window[e] = shifted(frames, e, W).astype(BF16)

    taps = jnp.concatenate([window[e, a * W : a * W + FX, :] for a in range(3) for e in range(3)], axis=1)
    for r in range(MID_ROWS):
        start = (MID_ROWS - 1 - r) * LAT_CH
        kernel = jnp.concatenate([padded[ae, start : start + LANES, :] for ae in range(9)], axis=0)
        pre = dot(taps, kernel) + first_bias_ref[...]
        inverse = lax.rsqrt(jnp.mean(pre * pre, axis=1, keepdims=True) + 1e-06)
        linear = pre * inverse * gain_ref[...]
        active = linear / (1.0 + jnp.exp(-linear))
        if r == 0:
            active = jnp.where(position == 0, 0.0, active)
        if r == MID_ROWS - 1:
            active = jnp.where(position == per_group - 1, 0.0, active)
        for t in range(FMAX):
            second[2 + t, r] = active[t * W : (t + 1) * W, :].astype(BF16)
    for copy in copies:
        copy.wait()

    @pl.when(position == 0)
    def _():
        second[0:2, 0] = jnp.zeros((2, W, MID_CH), BF16)

    @pl.when(position == per_group - 1)
    def _():
        second[0:2, MID_ROWS - 1] = jnp.zeros((2, W, MID_CH), BF16)

    ahead = pltpu.make_async_copy(second.at[pl.ds(live, 2), 1 : 1 + ROWS_DEV], next_ref, sems.at[0])
    ahead.start()

    width = W * LAT_CH
    kept = window[1, pl.ds(pl.multiple_of(live * W, W), 2 * W), :]
    own = iota((2 * W, width), 1) // LAT_CH == (iota((2 * W, width), 0) & (W - 1))
    for y in range(ROWS_DEV):
        pick = iota((LANES, width), 0) == (iota((LANES, width), 1) & (LAT_CH - 1)) + (HALO + y) * LAT_CH
        flat = jnp.where(own, dot(kept, pick.astype(F32).astype(BF16)), 0.0)
        for f in range(2):
            latent_ref[f, y : y + 1, :] = jnp.sum(flat[f * W : (f + 1) * W], axis=0, keepdims=True).astype(BF16)

    half = 2 * W
    pixels = ROWS_DEV * W
    diagonal = iota((OUT_CH, OUT_CH), 0) == iota((OUT_CH, OUT_CH), 1)
    bias = jnp.sum(jnp.where(diagonal, second_bias_ref[...], 0.0), axis=1, keepdims=True)
    column = iota((OUT_CH, pixels), 1) & (W - 1)
    at = iota((2 * half, 2 * half), 0)
    to = iota((2 * half, 2 * half), 1)
    source_row = (at & (half - 1)) // W
    weave = ((at & (W - 1)) * 2 + at // half + source_row * half == to).astype(F32).astype(BF16)
    sends = []
    for t in range(FMAX):
        for a in range(2):
            block = jnp.concatenate(
                [second[t + tau, a + i : a + i + ROWS_DEV].reshape(pixels, MID_CH) for tau in range(3) for i in range(2)],
                axis=1,
            )
            result = dot(weight[a], block, NT)
            left = pltpu.roll(result[2 * OUT_CH : 3 * OUT_CH], 1, 1)
            right = pltpu.roll(result[3 * OUT_CH : 4 * OUT_CH], pixels - 1, 1)
            even = result[0:OUT_CH] + jnp.where(column == 0, 0.0, left) + bias
            odd = result[OUT_CH : 2 * OUT_CH] + jnp.where(column == W - 1, 0.0, right) + bias
            even = jnp.where(t < live, even, 0.0).astype(BF16)
            odd = jnp.where(t < live, odd, 0.0).astype(BF16)
            for pair in range(ROWS_DEV // 2):
                lanes = slice(pair * half, (pair + 1) * half)
                woven = dot(jnp.concatenate([even[:, lanes], odd[:, lanes]], axis=1), weave).astype(BF16)
                for y in range(2):
                    decoded[t, 2 * (2 * pair + y) + a] = woven[:, y * half : (y + 1) * half]
        send = pltpu.make_async_copy(decoded.at[t], out_ref.at[t], out_sems.at[t])
        send.start()
        sends.append(send)
    for send in sends:
        send.wait()
    ahead.wait()


def body(
    latents,
    layout,
    assign,
    counts,
    latent_cache,
    feature_cache,
    first_weight,
    first_bias,
    norm_gain,
    second_weight,
    second_bias,
):
    devices = lax.axis_size("seq")
    slots = layout.shape[1]
    per_peer = slots // devices
    pairs = TILES * per_peer
    up = [(i, (i + 1) % devices) for i in range(devices)]
    down = [(j, i) for i, j in up]

    outgoing, last, first = pl.pallas_call(
        send_kernel,
        out_shape=(
            jax.ShapeDtypeStruct((devices, TILES * LANES), BF16),
            jax.ShapeDtypeStruct((2, W, MID_CH), BF16),
            jax.ShapeDtypeStruct((2, W, MID_CH), BF16),
        ),
        in_specs=[VMEM, VMEM, SMEM, ANY],
        out_specs=(VMEM, ANY, ANY),
        scratch_shapes=[pltpu.SemaphoreType.DMA((2,))],
        name="send",
    )(layout, latents, assign, feature_cache)
    latent_before = lax.ppermute(latent_cache, "seq", up)
    latent_after = lax.ppermute(latent_cache, "seq", down)
    feature_before = lax.ppermute(last, "seq", up)
    feature_after = lax.ppermute(first, "seq", down)
    incoming = lax.all_to_all(
        outgoing.reshape(devices, 1, TILES * LANES), "seq", split_axis=0, concat_axis=0, tiled=True
    ).reshape(devices, TILES * LANES)

    hot, codes, cached = pl.pallas_call(
        table_kernel,
        out_shape=(
            jax.ShapeDtypeStruct((FX, pairs * devices), BF16),
            jax.ShapeDtypeStruct((devices, LANES), F32),
            jax.ShapeDtypeStruct((2 * W, LANES), BF16),
        ),
        in_specs=[VMEM, SMEM, VMEM, VMEM, VMEM],
        out_specs=(VMEM, VMEM, VMEM),
        scratch_shapes=[pltpu.VMEM((WIN_ROWS * W, W * LAT_CH), BF16)],
        name="table",
    )(layout, assign, latent_cache, latent_before, latent_after)

    combined = pl.pallas_call(
        weight_kernel,
        grid=(3,),
        out_shape=jax.ShapeDtypeStruct((2, 4 * OUT_CH, 6 * MID_CH), BF16),
        in_specs=[pl.BlockSpec((1, 3, 3, OUT_CH, MID_CH), lambda t: (t, 0, 0, 0, 0))],
        out_specs=pl.BlockSpec((2, 4 * OUT_CH, 2 * MID_CH), lambda t: (0, 0, t)),
        name="combine",
    )(jnp.swapaxes(second_weight, 3, 4))

    decoded, latent_next, feature_next = pl.pallas_call(
        decode_kernel,
        out_shape=(
            jax.ShapeDtypeStruct((FMAX, 2 * ROWS_DEV, OUT_CH, 2 * W), BF16),
            jax.ShapeDtypeStruct((2, ROWS_DEV, W * LAT_CH), BF16),
            jax.ShapeDtypeStruct((2, ROWS_DEV, W, MID_CH), BF16),
        ),
        in_specs=[VMEM] * 4 + [SMEM] * 2 + [VMEM] * 4 + [ANY] * 4,
        out_specs=(ANY, VMEM, ANY),
        scratch_shapes=[
            pltpu.VMEM((2, 4 * OUT_CH, 6 * MID_CH), BF16),
            pltpu.VMEM((5, MID_ROWS, W, MID_CH), BF16),
            pltpu.VMEM((9, (2 * WIN_ROWS - 3) * LAT_CH, MID_CH), BF16),
            pltpu.VMEM((pairs * devices, LANES), BF16),
            pltpu.VMEM((3, 5 * W, LANES), BF16),
            pltpu.VMEM((FMAX, 2 * ROWS_DEV, OUT_CH, 2 * W), BF16),
            pltpu.SemaphoreType.DMA((4,)),
            pltpu.SemaphoreType.DMA((FMAX,)),
        ],
        name="decode",
    )(
        incoming,
        hot,
        codes,
        cached,
        assign,
        counts,
        first_weight,
        first_bias.reshape(1, MID_CH),
        norm_gain.reshape(1, MID_CH),
        second_bias.reshape(1, OUT_CH),
        feature_cache,
        feature_before,
        feature_after,
        combined,
    )
    return (jnp.swapaxes(decoded, 2, 3), latent_next, feature_next)


def solution(mesh):
    return jax.shard_map(
        body,
        mesh=mesh,
        in_specs=(
            P(None, ("rep", "seq")),
            P("rep", None),
            P("rep"),
            P("rep"),
            P(None, ("rep", "seq"), None),
            P(None, ("rep", "seq"), None, None),
            P(),
            P(),
            P(),
            P(),
            P(),
        ),
        out_specs=(
            P(None, ("rep", "seq"), None, None),
            P(None, ("rep", "seq"), None),
            P(None, ("rep", "seq"), None, None),
        ),
        check_vma=False,
    )
```

```python
import jax
import jax.numpy as jnp
from jax import lax
from jax.experimental import pallas as pl
from jax.experimental.pallas import tpu as pltpu
from jax.sharding import PartitionSpec as P

LAT_CH = 16
MID_CH = 384
OUT_CH = 192
REQS = 8
FMAX = 3
ROWS_DEV = 4
W = 64
LANES = 128
HALO = 2
WIN_ROWS = ROWS_DEV + 2 * HALO
MID_ROWS = ROWS_DEV + 2
FX = FMAX * W
TILES = 3
SLOTS = 4
PIECES = ((0, 384), (384, 768), (768, 1024))
BF16 = jnp.bfloat16
F32 = jnp.float32
I32 = jnp.int32
VMEM = pl.BlockSpec(memory_space=pltpu.VMEM)
SMEM = pl.BlockSpec(memory_space=pltpu.SMEM)
ANY = pl.BlockSpec(memory_space=pl.ANY)


def iota(shape, dim):
    return lax.broadcasted_iota(I32, shape, dim)


def dot(a, b, dims=((1,), (0,))):
    return lax.dot_general(a, b, (dims, ((), ())), preferred_element_type=F32)


NT = ((1,), (1,))


def cell_parts(numbers, assign_ref, devices):
    per_group = devices // REQS
    w_bits = W.bit_length() - 1
    height = ROWS_DEV * per_group
    h_bits = height.bit_length() - 1
    column = numbers & (W - 1)
    image_row = (numbers >> w_bits) & (height - 1)
    frames = numbers >> (w_bits + h_bits)
    request = jnp.zeros_like(frames)
    for r in range(1, REQS):
        request = request + (frames >= r * FMAX).astype(I32)
    frame = frames - request * FMAX
    group = jnp.zeros_like(frames)
    for g in range(1, REQS):
        group = jnp.where(request == assign_ref[g], g, group)
    place = group * per_group + image_row // ROWS_DEV
    target = (place - per_group // 2 + devices) & (devices - 1)
    return target, frame, image_row & (ROWS_DEV - 1), column


def earlier(length):
    return (iota((length, length), 0) < iota((length, length), 1)).astype(F32).astype(BF16)


def send_kernel(layout_ref, latents_ref, assign_ref, features_ref, cache_ref, out_ref, last_ref, first_ref, rows, wide, sems):
    devices, slots = layout_ref.shape
    per_peer = slots // devices
    me = lax.axis_index("seq")
    base = pl.multiple_of(me // 8 * 8, 8)
    copies = [
        pltpu.make_async_copy(layout_ref.at[pl.ds(base, 8)], rows, sems.at[0]),
        pltpu.make_async_copy(features_ref.at[:, ROWS_DEV - 1], last_ref.at[:, 0:W], sems.at[1]),
        pltpu.make_async_copy(features_ref.at[:, 0], first_ref.at[:, 0:W], sems.at[2]),
    ]
    for copy in copies:
        copy.start()
    for ref, top in ((last_ref, ROWS_DEV - HALO), (first_ref, 0)):
        for f in range(2):
            ref[f, W:, :] = jnp.zeros((ref.shape[1] - W, MID_CH), BF16)
            for y in range(HALO):
                for p, (low, high) in enumerate(PIECES):
                    at = W + y * len(PIECES) + p
                    ref[f, at : at + 1, 0 : high - low] = cache_ref[f, top + y : top + y + 1, low:high]
    order = earlier(slots)
    wide[...] = jnp.zeros(wide.shape, F32)
    copies[0].wait()
    own = jnp.sum(jnp.where(iota(rows.shape, 0) == me - base, rows[...], 0), axis=0, keepdims=True)
    target = cell_parts(own, assign_ref, devices)[0]
    member = (iota((devices, slots), 0) == target).astype(F32)
    rank = dot(member.astype(BF16), order)
    latents = latents_ref[...]
    out = jnp.zeros((devices, LANES), F32)
    for k in range(per_peer):
        picked = jnp.where(rank == float(k), member, 0.0).astype(BF16)
        cells = dot(picked, latents, NT).astype(BF16)
        spot = (iota((LAT_CH, LANES), 1) == iota((LAT_CH, LANES), 0) + k * LAT_CH).astype(F32)
        out = out + dot(cells, spot.astype(BF16))
    wide[pl.ds(0, devices, stride=SLOTS), :] = pltpu.roll(out, 1, 0)
    wide[pl.ds(1, devices, stride=SLOTS), :] = out
    wide[pl.ds(2, devices, stride=SLOTS), :] = pltpu.roll(out, devices - 1, 0)
    out_ref[...] = wide[...].astype(BF16)
    copies[1].wait()
    copies[2].wait()


def halo_line(ref, f, y):
    start = W + y * len(PIECES)
    parts = [ref[f, start + p : start + p + 1, 0 : high - low].astype(F32) for p, (low, high) in enumerate(PIECES)]
    return jnp.concatenate(parts, axis=1)


def table_kernel(layout_ref, assign_ref, cache_ref, before_ref, after_ref, hot_ref, code_ref, cached_ref, spread):
    devices, slots = layout_ref.shape
    per_group = devices // REQS
    per_peer = slots // devices
    me = lax.axis_index("seq")
    place = (me + per_group // 2) & (devices - 1)
    position = place & (per_group - 1)
    target, frame, row, column = cell_parts(layout_ref[...], assign_ref, devices)
    order = earlier(slots)
    codes = jnp.zeros((devices, LANES), F32)
    fx = frame * W + column
    lane = iota((devices, LANES), 1)
    for j in range(TILES):
        tile = (me + j - 1 + devices) & (devices - 1)
        hit = target == tile
        rank = dot(hit.astype(F32).astype(BF16), order)
        code = ((row + ROWS_DEV * j) * 256 + fx).astype(F32)
        if j == 0:
            code = jnp.where(position == 0, 0.0, code)
        if j == TILES - 1:
            code = jnp.where(position == per_group - 1, 0.0, code)
        code = jnp.where(hit, code, 0.0)
        for k in range(per_peer):
            one = jnp.sum(jnp.where(rank == float(k), code, 0.0), axis=1, keepdims=True)
            codes = jnp.where(lane == j * per_peer + k, one, codes)
    code_ref[...] = codes
    across = jnp.transpose(codes).astype(I32) & 255
    for jk in range(TILES * per_peer):
        hot = (iota((FX, devices), 0) == across[jk : jk + 1, :]).astype(F32)
        hot_ref[:, jk * devices : (jk + 1) * devices] = hot.astype(BF16)
    width = W * LAT_CH
    keep = iota((W, width), 1) // LAT_CH == iota((W, width), 0)
    repeat = ((iota((width, LANES), 0) & (LAT_CH - 1)) == (iota((width, LANES), 1) & (LAT_CH - 1))).astype(F32).astype(BF16)
    lane = iota((W, LANES), 1) // LAT_CH
    for f in range(2):
        for y in range(WIN_ROWS):
            if y < HALO:
                line = halo_line(before_ref, f, y)
                line = jnp.where(position == 0, 0.0, line)
            elif y < HALO + ROWS_DEV:
                line = cache_ref[f, y - HALO : y - HALO + 1, :].astype(F32)
            else:
                line = halo_line(after_ref, f, y - HALO - ROWS_DEV)
                line = jnp.where(position == per_group - 1, 0.0, line)
            spread[y * W : (y + 1) * W, :] = jnp.where(keep, line, 0.0).astype(BF16)
        wide = dot(spread[...], repeat)
        total = jnp.zeros((W, LANES), F32)
        for y in range(WIN_ROWS):
            total = jnp.where(lane == y, wide[y * W : (y + 1) * W, :], total)
        cached_ref[f * W : (f + 1) * W, :] = total.astype(BF16)


def weight_kernel(weight_ref, out_ref):
    taps = [[weight_ref[0, b, e].astype(F32) for e in range(3)] for b in range(3)]
    for a, i, rows in ((0, 0, (0,)), (0, 1, (1, 2)), (1, 0, (0, 1)), (1, 1, (2,))):
        line = [sum(taps[b][e] for b in rows[1:]) + taps[rows[0]][e] if len(rows) > 1 else taps[rows[0]][e] for e in range(3)]
        parts = (line[1] + line[2], line[0] + line[1], line[0], line[2])
        for g, part in enumerate(parts):
            out_ref[a, g * OUT_CH : (g + 1) * OUT_CH, i * MID_CH : (i + 1) * MID_CH] = part.astype(BF16)


def shifted(values, step, columns):
    if step == 1:
        return values
    rows = values.shape[0]
    x = iota(values.shape, 0) & (columns - 1)
    if step == 0:
        return jnp.where(x == 0, 0.0, pltpu.roll(values, 1, 0))
    return jnp.where(x == columns - 1, 0.0, pltpu.roll(values, rows - 1, 0))


def decode_kernel(
    incoming_ref,
    hot_ref,
    code_ref,
    cached_ref,
    assign_ref,
    counts_ref,
    first_weight_ref,
    first_bias_ref,
    gain_ref,
    second_bias_ref,
    features_ref,
    before_ref,
    after_ref,
    weight_ref,
    out_ref,
    latent_ref,
    next_ref,
    weight,
    second,
    padded,
    cells,
    window,
    received,
    halves,
    decoded,
    sems,
    out_sems,
):
    devices = lax.axis_size("seq")
    per_group = devices // REQS
    me = lax.axis_index("seq")
    place = (me + per_group // 2) & (devices - 1)
    position = place & (per_group - 1)
    live = counts_ref[assign_ref[place // per_group]]
    copies = [
        pltpu.make_async_copy(features_ref, second.at[0:2, 1 : 1 + ROWS_DEV], sems.at[0]),
        pltpu.make_async_copy(before_ref.at[:, 0:W], second.at[0:2, 0], sems.at[1]),
        pltpu.make_async_copy(after_ref.at[:, 0:W], second.at[0:2, MID_ROWS - 1], sems.at[2]),
        pltpu.make_async_copy(weight_ref, weight, sems.at[3]),
    ]
    for copy in copies:
        copy.start()

    margin = (WIN_ROWS - 3) * LAT_CH
    for a in range(3):
        for e in range(3):
            padded[a * 3 + e, 0:margin, :] = jnp.zeros((margin, MID_CH), BF16)
            padded[a * 3 + e, margin + 3 * LAT_CH :, :] = jnp.zeros((margin, MID_CH), BF16)
            for b in range(3):
                padded[a * 3 + e, margin + b * LAT_CH : margin + (b + 1) * LAT_CH, :] = first_weight_ref[a, b, e]

    pairs = hot_ref.shape[1] // devices
    per_peer = pairs // TILES
    wide = per_peer * LANES
    source = iota((LANES, wide), 1)
    expand = (iota((LANES, wide), 0) == source // LANES * LAT_CH + (source & (LAT_CH - 1))).astype(F32).astype(BF16)
    codes = code_ref[...].astype(I32) >> 8
    lane = iota((devices, LANES), 1) // LAT_CH + HALO
    received[...] = incoming_ref[...].astype(F32)
    for j in range(TILES):
        spread = dot(received[pl.ds(j, devices, stride=SLOTS), :].astype(BF16), expand)
        for k in range(per_peer):
            jk = j * per_peer + k
            part = jnp.where(lane == codes[:, jk : jk + 1], spread[:, k * LANES : (k + 1) * LANES], 0.0)
            cells[jk * devices : (jk + 1) * devices, :] = part.astype(BF16)
    arranged = dot(hot_ref[...], cells[...])
    frames = jnp.concatenate([cached_ref[...].astype(F32), arranged], axis=0)
    for e in range(3):
        window[e] = shifted(frames, e, W).astype(BF16)

    taps = jnp.concatenate([window[e, a * W : a * W + FX, :] for a in range(3) for e in range(3)], axis=1)
    for r in range(MID_ROWS):
        start = (MID_ROWS - 1 - r) * LAT_CH
        kernel = jnp.concatenate([padded[ae, start : start + LANES, :] for ae in range(9)], axis=0)
        pre = dot(taps, kernel) + first_bias_ref[...][None, :]
        inverse = lax.rsqrt(jnp.mean(pre * pre, axis=1, keepdims=True) + 1e-06)
        linear = pre * inverse * gain_ref[...][None, :]
        active = linear / (1.0 + jnp.exp(-linear))
        if r == 0:
            active = jnp.where(position == 0, 0.0, active)
        if r == MID_ROWS - 1:
            active = jnp.where(position == per_group - 1, 0.0, active)
        for t in range(FMAX):
            second[2 + t, r] = active[t * W : (t + 1) * W, :].astype(BF16)
    for copy in copies:
        copy.wait()

    @pl.when(position == 0)
    def _():
        second[0:2, 0] = jnp.zeros((2, W, MID_CH), BF16)

    @pl.when(position == per_group - 1)
    def _():
        second[0:2, MID_ROWS - 1] = jnp.zeros((2, W, MID_CH), BF16)

    ahead = pltpu.make_async_copy(second.at[pl.ds(live, 2), 1 : 1 + ROWS_DEV], next_ref, sems.at[0])
    ahead.start()

    width = W * LAT_CH
    kept = window[1, pl.ds(pl.multiple_of(live * W, W), 2 * W), :]
    own = iota((2 * W, width), 1) // LAT_CH == (iota((2 * W, width), 0) & (W - 1))
    for y in range(ROWS_DEV):
        pick = iota((LANES, width), 0) == (iota((LANES, width), 1) & (LAT_CH - 1)) + (HALO + y) * LAT_CH
        flat = jnp.where(own, dot(kept, pick.astype(F32).astype(BF16)), 0.0)
        for f in range(2):
            latent_ref[f, y : y + 1, :] = jnp.sum(flat[f * W : (f + 1) * W], axis=0, keepdims=True).astype(BF16)

    half = 2 * W
    pixels = ROWS_DEV * W
    diagonal = iota((OUT_CH, OUT_CH), 0) == iota((OUT_CH, OUT_CH), 1)
    bias = jnp.sum(jnp.where(diagonal, second_bias_ref[...][None, :], 0.0), axis=1, keepdims=True)
    column = iota((OUT_CH, pixels), 1) & (W - 1)
    for t in range(FMAX):
        for a in range(2):
            block = jnp.concatenate(
                [second[t + tau, a + i : a + i + ROWS_DEV].reshape(pixels, MID_CH) for tau in range(3) for i in range(2)],
                axis=1,
            )
            result = dot(weight[a], block, NT)
            left = pltpu.roll(result[2 * OUT_CH : 3 * OUT_CH], 1, 1)
            right = pltpu.roll(result[3 * OUT_CH : 4 * OUT_CH], pixels - 1, 1)
            even = result[0:OUT_CH] + jnp.where(column == 0, 0.0, left) + bias
            odd = result[OUT_CH : 2 * OUT_CH] + jnp.where(column == W - 1, 0.0, right) + bias
            even = jnp.where(t < live, even, 0.0).astype(BF16)
            odd = jnp.where(t < live, odd, 0.0).astype(BF16)
            for pair in range(ROWS_DEV // 2):
                lanes = slice(pair * half, (pair + 1) * half)
                at = (pair * 2 + a) * OUT_CH
                halves[t, at : at + OUT_CH, 0:half] = even[:, lanes]
                halves[t, at : at + OUT_CH, half : 2 * half] = odd[:, lanes]

    @pl.loop(0, FMAX)
    def _(t):
        at = iota((2 * half, 2 * half), 0)
        to = iota((2 * half, 2 * half), 1)
        source_row = (at & (half - 1)) // W
        weave = ((at & (W - 1)) * 2 + at // half + source_row * half == to).astype(F32).astype(BF16)
        woven = dot(halves[t], weave).astype(BF16)
        for pair in range(ROWS_DEV // 2):
            for a in range(2):
                start = (pair * 2 + a) * OUT_CH
                for y in range(2):
                    decoded[t, 2 * (2 * pair + y) + a] = woven[start : start + OUT_CH, y * half : (y + 1) * half]
        pltpu.make_async_copy(decoded.at[t], out_ref.at[t], out_sems.at[0]).start()

    pltpu.make_async_copy(decoded, out_ref, out_sems.at[0]).wait()
    ahead.wait()


def body(
    latents,
    layout,
    assign,
    counts,
    latent_cache,
    feature_cache,
    first_weight,
    first_bias,
    norm_gain,
    second_weight,
    second_bias,
):
    devices = lax.axis_size("seq")
    slots = layout.shape[1]
    per_peer = slots // devices
    pairs = TILES * per_peer
    up = [(i, (i + 1) % devices) for i in range(devices)]
    down = [(j, i) for i, j in up]

    edge = jax.ShapeDtypeStruct((2, W + 8, MID_CH), BF16)
    outgoing, last, first = pl.pallas_call(
        send_kernel,
        out_shape=(jax.ShapeDtypeStruct((devices * SLOTS, LANES), BF16), edge, edge),
        in_specs=[ANY, VMEM, SMEM, ANY, VMEM],
        out_specs=(VMEM, VMEM, VMEM),
        scratch_shapes=[
            pltpu.VMEM((8, slots), I32),
            pltpu.VMEM((devices * SLOTS, LANES), F32),
            pltpu.SemaphoreType.DMA((3,)),
        ],
        name="send",
    )(layout, latents, assign, feature_cache, latent_cache)
    before = lax.ppermute(last, "seq", up)
    after = lax.ppermute(first, "seq", down)
    incoming = lax.all_to_all(
        outgoing.reshape(devices, SLOTS, LANES), "seq", split_axis=0, concat_axis=0, tiled=True
    ).reshape(devices * SLOTS, LANES)

    hot, codes, cached = pl.pallas_call(
        table_kernel,
        out_shape=(
            jax.ShapeDtypeStruct((FX, pairs * devices), BF16),
            jax.ShapeDtypeStruct((devices, LANES), F32),
            jax.ShapeDtypeStruct((2 * W, LANES), BF16),
        ),
        in_specs=[VMEM, SMEM, VMEM, VMEM, VMEM],
        out_specs=(VMEM, VMEM, VMEM),
        scratch_shapes=[pltpu.VMEM((WIN_ROWS * W, W * LAT_CH), BF16)],
        name="table",
    )(layout, assign, latent_cache, before, after)

    combined = pl.pallas_call(
        weight_kernel,
        grid=(3,),
        out_shape=jax.ShapeDtypeStruct((2, 4 * OUT_CH, 6 * MID_CH), BF16),
        in_specs=[pl.BlockSpec((1, 3, 3, OUT_CH, MID_CH), lambda t: (t, 0, 0, 0, 0))],
        out_specs=pl.BlockSpec((2, 4 * OUT_CH, 2 * MID_CH), lambda t: (0, 0, t)),
        name="combine",
    )(jnp.swapaxes(second_weight, 3, 4))

    decoded, latent_next, feature_next = pl.pallas_call(
        decode_kernel,
        out_shape=(
            jax.ShapeDtypeStruct((FMAX, 2 * ROWS_DEV, OUT_CH, 2 * W), BF16),
            jax.ShapeDtypeStruct((2, ROWS_DEV, W * LAT_CH), BF16),
            jax.ShapeDtypeStruct((2, ROWS_DEV, W, MID_CH), BF16),
        ),
        in_specs=[VMEM] * 4 + [SMEM] * 2 + [VMEM] * 4 + [ANY] * 4,
        out_specs=(ANY, VMEM, ANY),
        scratch_shapes=[
            pltpu.VMEM((2, 4 * OUT_CH, 6 * MID_CH), BF16),
            pltpu.VMEM((5, MID_ROWS, W, MID_CH), BF16),
            pltpu.VMEM((9, (2 * WIN_ROWS - 3) * LAT_CH, MID_CH), BF16),
            pltpu.VMEM((pairs * devices, LANES), BF16),
            pltpu.VMEM((3, 5 * W, LANES), BF16),
            pltpu.VMEM((devices * SLOTS, LANES), F32),
            pltpu.VMEM((FMAX, ROWS_DEV * OUT_CH, 4 * W), BF16),
            pltpu.VMEM((FMAX, 2 * ROWS_DEV, OUT_CH, 2 * W), BF16),
            pltpu.SemaphoreType.DMA((4,)),
            pltpu.SemaphoreType.DMA((1,)),
        ],
        name="decode",
    )(
        incoming,
        hot,
        codes,
        cached,
        assign,
        counts,
        first_weight,
        first_bias,
        norm_gain,
        second_bias,
        feature_cache,
        before,
        after,
        combined,
    )
    return (jnp.swapaxes(decoded, 2, 3), latent_next, feature_next)


def solution(mesh):
    return jax.shard_map(
        body,
        mesh=mesh,
        in_specs=(
            P(None, ("rep", "seq")),
            P("rep", None),
            P("rep"),
            P("rep"),
            P(None, ("rep", "seq"), None),
            P(None, ("rep", "seq"), None, None),
            P(),
            P(),
            P(),
            P(),
            P(),
        ),
        out_specs=(
            P(None, ("rep", "seq"), None, None),
            P(None, ("rep", "seq"), None),
            P(None, ("rep", "seq"), None, None),
        ),
        check_vma=False,
    )
```

```python
import jax
import jax.numpy as jnp
from jax import lax
from jax.experimental import pallas as pl
from jax.experimental.pallas import tpu as pltpu
from jax.sharding import PartitionSpec as P

LAT_CH = 16
MID_CH = 384
OUT_CH = 192
REQS = 8
FMAX = 3
ROWS_DEV = 4
W = 64
LANES = 128
HALO = 2
WIN_ROWS = ROWS_DEV + 2 * HALO
MID_ROWS = ROWS_DEV + 2
FX = FMAX * W
TILES = 3
SLOTS = 4
PIECES = ((0, 384), (384, 768), (768, 1024))
BF16 = jnp.bfloat16
F32 = jnp.float32
I32 = jnp.int32
VMEM = pl.BlockSpec(memory_space=pltpu.VMEM)
SMEM = pl.BlockSpec(memory_space=pltpu.SMEM)
ANY = pl.BlockSpec(memory_space=pl.ANY)


def iota(shape, dim):
    return lax.broadcasted_iota(I32, shape, dim)


def dot(a, b, dims=((1,), (0,))):
    return lax.dot_general(a, b, (dims, ((), ())), preferred_element_type=F32)


NT = ((1,), (1,))


def cell_parts(numbers, assign_ref, devices):
    per_group = devices // REQS
    w_bits = W.bit_length() - 1
    height = ROWS_DEV * per_group
    h_bits = height.bit_length() - 1
    column = numbers & (W - 1)
    image_row = (numbers >> w_bits) & (height - 1)
    frames = numbers >> (w_bits + h_bits)
    request = jnp.zeros_like(frames)
    for r in range(1, REQS):
        request = request + (frames >= r * FMAX).astype(I32)
    frame = frames - request * FMAX
    group = jnp.zeros_like(frames)
    for g in range(1, REQS):
        group = jnp.where(request == assign_ref[g], g, group)
    place = group * per_group + image_row // ROWS_DEV
    target = (place - per_group // 2 + devices) & (devices - 1)
    return target, frame, image_row & (ROWS_DEV - 1), column


def earlier(length):
    return (iota((length, length), 0) < iota((length, length), 1)).astype(F32).astype(BF16)


def send_kernel(layout_ref, latents_hbm, assign_ref, features_ref, cache_hbm, out_ref, last_ref, first_ref, rows, latents_ref, cache_ref, wide, sems):
    devices, slots = layout_ref.shape
    per_peer = slots // devices
    me = lax.axis_index("seq")
    base = pl.multiple_of(me // 8 * 8, 8)
    copies = [
        pltpu.make_async_copy(layout_ref.at[pl.ds(base, 8)], rows, sems.at[0]),
        pltpu.make_async_copy(features_ref.at[:, ROWS_DEV - 1], last_ref.at[:, 0:W], sems.at[1]),
        pltpu.make_async_copy(features_ref.at[:, 0], first_ref.at[:, 0:W], sems.at[2]),
        pltpu.make_async_copy(latents_hbm, latents_ref, sems.at[3]),
        pltpu.make_async_copy(cache_hbm, cache_ref, sems.at[4]),
    ]
    for copy in copies:
        copy.start()
    order = earlier(slots)
    wide[...] = jnp.zeros(wide.shape, F32)
    copies[4].wait()
    for ref, top in ((last_ref, ROWS_DEV - HALO), (first_ref, 0)):
        for f in range(2):
            ref[f, W:, :] = jnp.zeros((ref.shape[1] - W, MID_CH), BF16)
            for y in range(HALO):
                for p, (low, high) in enumerate(PIECES):
                    at = W + y * len(PIECES) + p
                    ref[f, at : at + 1, 0 : high - low] = cache_ref[f, top + y : top + y + 1, low:high]
    copies[0].wait()
    own = jnp.sum(jnp.where(iota(rows.shape, 0) == me - base, rows[...], 0), axis=0, keepdims=True)
    target = cell_parts(own, assign_ref, devices)[0]
    member = (iota((devices, slots), 0) == target).astype(F32)
    rank = dot(member.astype(BF16), order)
    copies[3].wait()
    latents = latents_ref[...]
    out = jnp.zeros((devices, LANES), F32)
    for k in range(per_peer):
        picked = jnp.where(rank == float(k), member, 0.0).astype(BF16)
        cells = dot(picked, latents, NT).astype(BF16)
        spot = (iota((LAT_CH, LANES), 1) == iota((LAT_CH, LANES), 0) + k * LAT_CH).astype(F32)
        out = out + dot(cells, spot.astype(BF16))
    wide[pl.ds(0, devices, stride=SLOTS), :] = pltpu.roll(out, 1, 0)
    wide[pl.ds(1, devices, stride=SLOTS), :] = out
    wide[pl.ds(2, devices, stride=SLOTS), :] = pltpu.roll(out, devices - 1, 0)
    out_ref[...] = wide[...].astype(BF16)
    copies[1].wait()
    copies[2].wait()


def halo_line(ref, f, y):
    start = W + y * len(PIECES)
    parts = [ref[f, start + p : start + p + 1, 0 : high - low].astype(F32) for p, (low, high) in enumerate(PIECES)]
    return jnp.concatenate(parts, axis=1)


def table_kernel(layout_ref, assign_ref, cache_ref, before_ref, after_ref, across_ref, code_ref, cached_ref, spread):
    devices, slots = layout_ref.shape
    per_group = devices // REQS
    per_peer = slots // devices
    me = lax.axis_index("seq")
    place = (me + per_group // 2) & (devices - 1)
    position = place & (per_group - 1)
    target, frame, row, column = cell_parts(layout_ref[...], assign_ref, devices)
    order = earlier(slots)
    codes = jnp.zeros((devices, LANES), F32)
    fx = frame * W + column
    lane = iota((devices, LANES), 1)
    for j in range(TILES):
        tile = (me + j - 1 + devices) & (devices - 1)
        hit = target == tile
        rank = dot(hit.astype(F32).astype(BF16), order)
        code = ((row + ROWS_DEV * j) * 256 + fx).astype(F32)
        if j == 0:
            code = jnp.where(position == 0, 0.0, code)
        if j == TILES - 1:
            code = jnp.where(position == per_group - 1, 0.0, code)
        code = jnp.where(hit, code, 0.0)
        for k in range(per_peer):
            one = jnp.sum(jnp.where(rank == float(k), code, 0.0), axis=1, keepdims=True)
            codes = jnp.where(lane == j * per_peer + k, one, codes)
    code_ref[...] = codes
    across_ref[...] = jnp.transpose(codes).astype(I32) & 255
    width = W * LAT_CH
    keep = iota((W, width), 1) // LAT_CH == iota((W, width), 0)
    repeat = ((iota((width, LANES), 0) & (LAT_CH - 1)) == (iota((width, LANES), 1) & (LAT_CH - 1))).astype(F32).astype(BF16)
    lane = iota((W, LANES), 1) // LAT_CH
    for f in range(2):
        for y in range(WIN_ROWS):
            if y < HALO:
                line = halo_line(before_ref, f, y)
                line = jnp.where(position == 0, 0.0, line)
            elif y < HALO + ROWS_DEV:
                line = cache_ref[f, y - HALO : y - HALO + 1, :].astype(F32)
            else:
                line = halo_line(after_ref, f, y - HALO - ROWS_DEV)
                line = jnp.where(position == per_group - 1, 0.0, line)
            spread[y * W : (y + 1) * W, :] = jnp.where(keep, line, 0.0).astype(BF16)
        wide = dot(spread[...], repeat)
        total = jnp.zeros((W, LANES), F32)
        for y in range(WIN_ROWS):
            total = jnp.where(lane == y, wide[y * W : (y + 1) * W, :], total)
        cached_ref[f * W : (f + 1) * W, :] = total.astype(BF16)


def weight_kernel(weight_ref, out_ref, raw, sums, sems, out_sems):
    copies = [pltpu.make_async_copy(weight_ref.at[tau], raw.at[tau], sems.at[tau]) for tau in range(3)]
    for copy in copies:
        copy.start()
    sends = []
    for tau in range(3):
        copies[tau].wait()
        lanes = pl.ds(tau * 2 * MID_CH, 2 * MID_CH)
        for a in range(2):
            for i, rows in enumerate((((0,), (1, 2)), ((0, 1), (2,)))[a]):
                line = [sum((raw[tau, b, e].astype(F32) for b in rows[1:]), raw[tau, rows[0], e].astype(F32)) for e in range(3)]
                parts = (line[1] + line[2], line[0] + line[1], line[0], line[2])
                at = (tau * 2 + i) * MID_CH
                for g, part in enumerate(parts):
                    sums[a, g * OUT_CH : (g + 1) * OUT_CH, at : at + MID_CH] = part.astype(BF16)
            send = pltpu.make_async_copy(sums.at[a, :, lanes], out_ref.at[a, :, lanes], out_sems.at[tau * 2 + a])
            send.start()
            sends.append(send)
    for send in sends:
        send.wait()


def shifted(values, step, columns):
    if step == 1:
        return values
    rows = values.shape[0]
    x = iota(values.shape, 0) & (columns - 1)
    if step == 0:
        return jnp.where(x == 0, 0.0, pltpu.roll(values, 1, 0))
    return jnp.where(x == columns - 1, 0.0, pltpu.roll(values, rows - 1, 0))


def decode_kernel(
    incoming_ref,
    across_ref,
    code_ref,
    cached_ref,
    assign_ref,
    counts_ref,
    first_hbm,
    first_bias_ref,
    gain_ref,
    second_bias_ref,
    features_ref,
    before_ref,
    after_ref,
    weight_ref,
    out_ref,
    latent_ref,
    next_ref,
    first_weight_ref,
    weave_ref,
    weight,
    second,
    padded,
    cells,
    window,
    received,
    halves,
    decoded,
    sems,
    out_sems,
):
    devices = lax.axis_size("seq")
    per_group = devices // REQS
    me = lax.axis_index("seq")
    place = (me + per_group // 2) & (devices - 1)
    position = place & (per_group - 1)
    live = counts_ref[assign_ref[place // per_group]]
    copies = [
        pltpu.make_async_copy(features_ref, second.at[0:2, 1 : 1 + ROWS_DEV], sems.at[0]),
        pltpu.make_async_copy(first_hbm, first_weight_ref, sems.at[1]),
        pltpu.make_async_copy(weight_ref.at[0], weight.at[0], sems.at[2]),
        pltpu.make_async_copy(weight_ref.at[1], weight.at[1], sems.at[3]),
    ]
    for copy in copies:
        copy.start()

    half = 2 * W
    at = iota((2 * half, 2 * half), 0)
    source_row = (at & (half - 1)) // W
    target = (at & (W - 1)) * 2 + at // half + source_row * half
    weave_ref[...] = (target == iota((2 * half, 2 * half), 1)).astype(F32).astype(BF16)

    per_peer = FX * ROWS_DEV // devices
    pairs = TILES * per_peer
    hot = jnp.concatenate(
        [(iota((FX, devices), 0) == across_ref[jk : jk + 1, :]).astype(F32).astype(BF16) for jk in range(pairs)], axis=1
    )
    wide = per_peer * LANES
    source = iota((LANES, wide), 1)
    expand = (iota((LANES, wide), 0) == source // LANES * LAT_CH + (source & (LAT_CH - 1))).astype(F32).astype(BF16)
    codes = code_ref[...].astype(I32) >> 8
    lane = iota((devices, LANES), 1) // LAT_CH + HALO
    received[...] = incoming_ref[...].astype(F32)
    for j in range(TILES):
        spread = dot(received[pl.ds(j, devices, stride=SLOTS), :].astype(BF16), expand)
        for k in range(per_peer):
            jk = j * per_peer + k
            part = jnp.where(lane == codes[:, jk : jk + 1], spread[:, k * LANES : (k + 1) * LANES], 0.0)
            cells[jk * devices : (jk + 1) * devices, :] = part.astype(BF16)
    arranged = dot(hot, cells[...])
    frames = jnp.concatenate([cached_ref[...].astype(F32), arranged], axis=0)
    for e in range(3):
        window[e] = shifted(frames, e, W).astype(BF16)

    copies[1].wait()
    margin = (WIN_ROWS - 3) * LAT_CH
    for a in range(3):
        for e in range(3):
            padded[a * 3 + e, 0:margin, :] = jnp.zeros((margin, MID_CH), BF16)
            padded[a * 3 + e, margin + 3 * LAT_CH :, :] = jnp.zeros((margin, MID_CH), BF16)
            for b in range(3):
                padded[a * 3 + e, margin + b * LAT_CH : margin + (b + 1) * LAT_CH, :] = first_weight_ref[a, b, e]

    taps = jnp.concatenate([window[e, a * W : a * W + FX, :] for a in range(3) for e in range(3)], axis=1)
    for r in range(MID_ROWS):
        start = (MID_ROWS - 1 - r) * LAT_CH
        kernel = jnp.concatenate([padded[ae, start : start + LANES, :] for ae in range(9)], axis=0)
        pre = dot(taps, kernel) + first_bias_ref[...][None, :]
        inverse = lax.rsqrt(jnp.mean(pre * pre, axis=1, keepdims=True) + 1e-06)
        linear = pre * inverse * gain_ref[...][None, :]
        active = linear / (1.0 + jnp.exp(-linear))
        if r == 0:
            active = jnp.where(position == 0, 0.0, active)
        if r == MID_ROWS - 1:
            active = jnp.where(position == per_group - 1, 0.0, active)
        for t in range(FMAX):
            second[2 + t, r] = active[t * W : (t + 1) * W, :].astype(BF16)
    for f in range(2):
        edge = before_ref[f, 0:W, :]
        second[f, 0] = jnp.where(position == 0, jnp.zeros_like(edge), edge)
        edge = after_ref[f, 0:W, :]
        second[f, MID_ROWS - 1] = jnp.where(position == per_group - 1, jnp.zeros_like(edge), edge)
    copies[0].wait()
    ahead = pltpu.make_async_copy(second.at[pl.ds(live, 2), 1 : 1 + ROWS_DEV], next_ref, sems.at[0])
    ahead.start()

    width = W * LAT_CH
    kept = window[1, pl.ds(pl.multiple_of(live * W, W), 2 * W), :]
    own = iota((2 * W, width), 1) // LAT_CH == (iota((2 * W, width), 0) & (W - 1))
    for y in range(ROWS_DEV):
        pick = iota((LANES, width), 0) == (iota((LANES, width), 1) & (LAT_CH - 1)) + (HALO + y) * LAT_CH
        flat = jnp.where(own, dot(kept, pick.astype(F32).astype(BF16)), 0.0)
        for f in range(2):
            latent_ref[f, y : y + 1, :] = jnp.sum(flat[f * W : (f + 1) * W], axis=0, keepdims=True).astype(BF16)

    pixels = ROWS_DEV * W
    diagonal = iota((OUT_CH, OUT_CH), 0) == iota((OUT_CH, OUT_CH), 1)
    bias = jnp.sum(jnp.where(diagonal, second_bias_ref[...][None, :], 0.0), axis=1, keepdims=True)
    column = iota((OUT_CH, pixels), 1) & (W - 1)
    def interleave(a):
        woven = dot(halves[a], weave_ref[...]).astype(BF16)
        for t in range(FMAX):
            for pair in range(ROWS_DEV // 2):
                start = (t * (ROWS_DEV // 2) + pair) * OUT_CH
                for y in range(2):
                    decoded[a, t, 2 * pair + y] = woven[start : start + OUT_CH, y * half : (y + 1) * half]
        pltpu.make_async_copy(decoded.at[a], out_ref.at[:, :, a], out_sems.at[a]).start()

    for a in range(2):
        copies[2 + a].wait()
        for t in range(FMAX):
            block = jnp.concatenate(
                [second[t + tau, a + i : a + i + ROWS_DEV].reshape(pixels, MID_CH) for tau in range(3) for i in range(2)],
                axis=1,
            )
            result = dot(weight[a], block, NT)
            left = pltpu.roll(result[2 * OUT_CH : 3 * OUT_CH], 1, 1)
            right = pltpu.roll(result[3 * OUT_CH : 4 * OUT_CH], pixels - 1, 1)
            even = result[0:OUT_CH] + jnp.where(column == 0, 0.0, left) + bias
            odd = result[OUT_CH : 2 * OUT_CH] + jnp.where(column == W - 1, 0.0, right) + bias
            even = jnp.where(t < live, even, 0.0).astype(BF16)
            odd = jnp.where(t < live, odd, 0.0).astype(BF16)
            for pair in range(ROWS_DEV // 2):
                lanes = slice(pair * half, (pair + 1) * half)
                start = (t * (ROWS_DEV // 2) + pair) * OUT_CH
                halves[a, start : start + OUT_CH, 0:half] = even[:, lanes]
                halves[a, start : start + OUT_CH, half : 2 * half] = odd[:, lanes]
        pl.when(live >= 0)(lambda a=a: interleave(a))
    for a in range(2):
        pltpu.make_async_copy(decoded.at[a], out_ref.at[:, :, a], out_sems.at[a]).wait()
    ahead.wait()


def in_vmem(array):
    return pltpu.with_memory_space_constraint(array, pltpu.VMEM)


def body(
    latents,
    layout,
    assign,
    counts,
    latent_cache,
    feature_cache,
    first_weight,
    first_bias,
    norm_gain,
    second_weight,
    second_bias,
):
    devices = lax.axis_size("seq")
    slots = layout.shape[1]
    per_peer = slots // devices
    pairs = TILES * per_peer
    up = [(i, (i + 1) % devices) for i in range(devices)]
    down = [(j, i) for i, j in up]

    edge = jax.ShapeDtypeStruct((2, W + 8, MID_CH), BF16)
    outgoing, last, first = pl.pallas_call(
        send_kernel,
        out_shape=(jax.ShapeDtypeStruct((devices * SLOTS, LANES), BF16), edge, edge),
        in_specs=[ANY, ANY, SMEM, ANY, ANY],
        out_specs=(VMEM, VMEM, VMEM),
        scratch_shapes=[
            pltpu.VMEM((8, slots), I32),
            pltpu.VMEM(latents.shape, BF16),
            pltpu.VMEM(latent_cache.shape, BF16),
            pltpu.VMEM((devices * SLOTS, LANES), F32),
            pltpu.SemaphoreType.DMA((5,)),
        ],
        name="send",
    )(layout, latents, assign, feature_cache, latent_cache)
    before = in_vmem(lax.ppermute(last, "seq", up))
    after = in_vmem(lax.ppermute(first, "seq", down))
    incoming = lax.all_to_all(
        outgoing.reshape(devices, SLOTS, LANES), "seq", split_axis=0, concat_axis=0, tiled=True
    ).reshape(devices * SLOTS, LANES)

    across, codes, cached = pl.pallas_call(
        table_kernel,
        out_shape=(
            pltpu.VMEM((LANES, devices), I32),
            pltpu.VMEM((devices, LANES), F32),
            pltpu.VMEM((2 * W, LANES), BF16),
        ),
        in_specs=[VMEM, SMEM, VMEM, VMEM, VMEM],
        out_specs=(VMEM, VMEM, VMEM),
        scratch_shapes=[pltpu.VMEM((WIN_ROWS * W, W * LAT_CH), BF16)],
        name="table",
    )(layout, assign, latent_cache, before, after)

    combined = pl.pallas_call(
        weight_kernel,
        out_shape=jax.ShapeDtypeStruct((2, 4 * OUT_CH, 6 * MID_CH), BF16),
        in_specs=[ANY],
        out_specs=ANY,
        scratch_shapes=[
            pltpu.VMEM((3, 3, 3, OUT_CH, MID_CH), BF16),
            pltpu.VMEM((2, 4 * OUT_CH, 6 * MID_CH), BF16),
            pltpu.SemaphoreType.DMA((3,)),
            pltpu.SemaphoreType.DMA((6,)),
        ],
        name="combine",
    )(jnp.swapaxes(second_weight, 3, 4))

    decoded, latent_next, feature_next = pl.pallas_call(
        decode_kernel,
        out_shape=(
            jax.ShapeDtypeStruct((FMAX, ROWS_DEV, 2, OUT_CH, 2 * W), BF16),
            jax.ShapeDtypeStruct((2, ROWS_DEV, W * LAT_CH), BF16),
            jax.ShapeDtypeStruct((2, ROWS_DEV, W, MID_CH), BF16),
        ),
        in_specs=[VMEM] * 4 + [SMEM] * 2 + [ANY] + [VMEM] * 3 + [ANY] + [VMEM] * 2 + [ANY],
        out_specs=(ANY, VMEM, ANY),
        scratch_shapes=[
            pltpu.VMEM(first_weight.shape, BF16),
            pltpu.VMEM((4 * W, 4 * W), BF16),
            pltpu.VMEM((2, 4 * OUT_CH, 6 * MID_CH), BF16),
            pltpu.VMEM((5, MID_ROWS, W, MID_CH), BF16),
            pltpu.VMEM((9, (2 * WIN_ROWS - 3) * LAT_CH, MID_CH), BF16),
            pltpu.VMEM((pairs * devices, LANES), BF16),
            pltpu.VMEM((3, 5 * W, LANES), BF16),
            pltpu.VMEM((devices * SLOTS, LANES), F32),
            pltpu.VMEM((2, FMAX * (ROWS_DEV // 2) * OUT_CH, 4 * W), BF16),
            pltpu.VMEM((2, FMAX, ROWS_DEV, OUT_CH, 2 * W), BF16),
            pltpu.SemaphoreType.DMA((4,)),
            pltpu.SemaphoreType.DMA((2,)),
        ],
        name="decode",
    )(
        in_vmem(incoming),
        in_vmem(across),
        in_vmem(codes),
        in_vmem(cached),
        assign,
        counts,
        first_weight,
        first_bias,
        norm_gain,
        second_bias,
        feature_cache,
        before,
        after,
        combined,
    )
    decoded = decoded.reshape(FMAX, 2 * ROWS_DEV, OUT_CH, 2 * W)
    return (jnp.swapaxes(decoded, 2, 3), latent_next, feature_next)


def solution(mesh):
    return jax.shard_map(
        body,
        mesh=mesh,
        in_specs=(
            P(None, ("rep", "seq")),
            P("rep", None),
            P("rep"),
            P("rep"),
            P(None, ("rep", "seq"), None),
            P(None, ("rep", "seq"), None, None),
            P(),
            P(),
            P(),
            P(),
            P(),
        ),
        out_specs=(
            P(None, ("rep", "seq"), None, None),
            P(None, ("rep", "seq"), None),
            P(None, ("rep", "seq"), None, None),
        ),
        check_vma=False,
    )
```

```python
import jax
import jax.numpy as jnp
from jax import lax
from jax.experimental import pallas as pl
from jax.experimental.pallas import tpu as pltpu
from jax.sharding import PartitionSpec as P

LAT_CH = 16
MID_CH = 384
OUT_CH = 192
REQS = 8
FMAX = 3
ROWS_DEV = 4
W = 64
LANES = 128
HALO = 2
WIN_ROWS = ROWS_DEV + 2 * HALO
MID_ROWS = ROWS_DEV + 2
FX = FMAX * W
TILES = 3
SLOTS = 4
PIECES = ((0, 384), (384, 768), (768, 1024))
BF16 = jnp.bfloat16
F32 = jnp.float32
I32 = jnp.int32
VMEM = pl.BlockSpec(memory_space=pltpu.VMEM)
SMEM = pl.BlockSpec(memory_space=pltpu.SMEM)
ANY = pl.BlockSpec(memory_space=pl.ANY)


def iota(shape, dim):
    return lax.broadcasted_iota(I32, shape, dim)


def dot(a, b, dims=((1,), (0,))):
    return lax.dot_general(a, b, (dims, ((), ())), preferred_element_type=F32)


NT = ((1,), (1,))


def cell_parts(numbers, assign_ref, devices):
    per_group = devices // REQS
    w_bits = W.bit_length() - 1
    height = ROWS_DEV * per_group
    h_bits = height.bit_length() - 1
    column = numbers & (W - 1)
    image_row = (numbers >> w_bits) & (height - 1)
    frames = numbers >> (w_bits + h_bits)
    request = (frames * 11) >> 5
    frame = frames - request * FMAX
    group_of = jnp.int32(0)
    for g in range(1, REQS):
        group_of = group_of + (jnp.int32(g) << (assign_ref[g] * 4))
    group = (group_of >> (request * 4)) & (REQS - 1)
    place = group * per_group + image_row // ROWS_DEV
    target = (place - per_group // 2 + devices) & (devices - 1)
    return target, frame, image_row & (ROWS_DEV - 1), column


def earlier(length):
    return (iota((length, length), 0) < iota((length, length), 1)).astype(F32).astype(BF16)


def send_kernel(
    layout_ref, latents_hbm, assign_hbm, features_ref, cache_hbm, out_ref, last_ref, first_ref, rows, latents_ref, cache_ref, assign_ref, wide, sems
):
    devices, slots = layout_ref.shape
    per_peer = slots // devices
    me = lax.axis_index("seq")
    base = pl.multiple_of(me // 8 * 8, 8)
    copies = [
        pltpu.make_async_copy(layout_ref.at[pl.ds(base, 8)], rows, sems.at[0]),
        pltpu.make_async_copy(features_ref.at[:, ROWS_DEV - 1], last_ref.at[:, 0:W], sems.at[1]),
        pltpu.make_async_copy(features_ref.at[:, 0], first_ref.at[:, 0:W], sems.at[2]),
        pltpu.make_async_copy(latents_hbm, latents_ref, sems.at[3]),
        pltpu.make_async_copy(cache_hbm, cache_ref, sems.at[4]),
        pltpu.make_async_copy(assign_hbm, assign_ref, sems.at[5]),
    ]
    for copy in copies:
        copy.start()
    order = earlier(slots)
    wide[...] = jnp.zeros(wide.shape, F32)
    copies[4].wait()
    for ref, top in ((last_ref, ROWS_DEV - HALO), (first_ref, 0)):
        for f in range(2):
            ref[f, W:, :] = jnp.zeros((ref.shape[1] - W, MID_CH), BF16)
            for y in range(HALO):
                for p, (low, high) in enumerate(PIECES):
                    at = W + y * len(PIECES) + p
                    ref[f, at : at + 1, 0 : high - low] = cache_ref[f, top + y : top + y + 1, low:high]
    copies[0].wait()
    copies[5].wait()
    own = jnp.sum(jnp.where(iota(rows.shape, 0) == me - base, rows[...], 0), axis=0, keepdims=True)
    target = cell_parts(own, assign_ref, devices)[0]
    member = (iota((devices, slots), 0) == target).astype(F32)
    rank = dot(member.astype(BF16), order)
    copies[3].wait()
    latents = latents_ref[...]
    out = jnp.zeros((devices, LANES), F32)
    for k in range(per_peer):
        picked = jnp.where(rank == float(k), member, 0.0).astype(BF16)
        cells = dot(picked, latents, NT).astype(BF16)
        spot = (iota((LAT_CH, LANES), 1) == iota((LAT_CH, LANES), 0) + k * LAT_CH).astype(F32)
        out = out + dot(cells, spot.astype(BF16))
    wide[pl.ds(0, devices, stride=SLOTS), :] = pltpu.roll(out, 1, 0)
    wide[pl.ds(1, devices, stride=SLOTS), :] = out
    wide[pl.ds(2, devices, stride=SLOTS), :] = pltpu.roll(out, devices - 1, 0)
    out_ref[...] = wide[...].astype(BF16)
    copies[1].wait()
    copies[2].wait()


def halo_line(ref, f, y):
    start = W + y * len(PIECES)
    parts = [ref[f, start + p : start + p + 1, 0 : high - low].astype(F32) for p, (low, high) in enumerate(PIECES)]
    return jnp.concatenate(parts, axis=1)


def table_kernel(layout_ref, assign_ref, cache_ref, before_ref, after_ref, across_ref, code_ref, cached_ref, spread):
    devices, slots = layout_ref.shape
    per_group = devices // REQS
    per_peer = slots // devices
    me = lax.axis_index("seq")
    place = (me + per_group // 2) & (devices - 1)
    position = place & (per_group - 1)
    target, frame, row, column = cell_parts(layout_ref[...], assign_ref, devices)
    order = earlier(slots)
    codes = jnp.zeros((devices, LANES), F32)
    fx = frame * W + column
    lane = iota((devices, LANES), 1)
    for j in range(TILES):
        tile = (me + j - 1 + devices) & (devices - 1)
        hit = target == tile
        rank = dot(hit.astype(F32).astype(BF16), order)
        code = ((row + ROWS_DEV * j) * 256 + fx).astype(F32)
        if j == 0:
            code = jnp.where(position == 0, 0.0, code)
        if j == TILES - 1:
            code = jnp.where(position == per_group - 1, 0.0, code)
        code = jnp.where(hit, code, 0.0)
        for k in range(per_peer):
            one = jnp.sum(jnp.where(rank == float(k), code, 0.0), axis=1, keepdims=True)
            codes = jnp.where(lane == j * per_peer + k, one, codes)
    code_ref[...] = codes
    across_ref[...] = jnp.transpose(codes).astype(I32) & 255
    width = W * LAT_CH
    keep = iota((W, width), 1) // LAT_CH == iota((W, width), 0)
    repeat = ((iota((width, LANES), 0) & (LAT_CH - 1)) == (iota((width, LANES), 1) & (LAT_CH - 1))).astype(F32).astype(BF16)
    lane = iota((W, LANES), 1) // LAT_CH
    for f in range(2):
        for y in range(WIN_ROWS):
            if y < HALO:
                line = halo_line(before_ref, f, y)
                line = jnp.where(position == 0, 0.0, line)
            elif y < HALO + ROWS_DEV:
                line = cache_ref[f, y - HALO : y - HALO + 1, :].astype(F32)
            else:
                line = halo_line(after_ref, f, y - HALO - ROWS_DEV)
                line = jnp.where(position == per_group - 1, 0.0, line)
            spread[y * W : (y + 1) * W, :] = jnp.where(keep, line, 0.0).astype(BF16)
        wide = dot(spread[...], repeat)
        total = jnp.zeros((W, LANES), F32)
        for y in range(WIN_ROWS):
            total = jnp.where(lane == y, wide[y * W : (y + 1) * W, :], total)
        cached_ref[f * W : (f + 1) * W, :] = total.astype(BF16)


def weight_kernel(weight_ref, out_ref, raw, sums, sems, out_sems):
    copies = [pltpu.make_async_copy(weight_ref.at[tau], raw.at[tau], sems.at[tau]) for tau in range(3)]
    for copy in copies:
        copy.start()
    sends = []
    for tau in range(3):
        copies[tau].wait()
        lanes = pl.ds(tau * 2 * MID_CH, 2 * MID_CH)
        for a in range(2):
            for i, rows in enumerate((((0,), (1, 2)), ((0, 1), (2,)))[a]):
                line = [sum((raw[tau, b, e].astype(F32) for b in rows[1:]), raw[tau, rows[0], e].astype(F32)) for e in range(3)]
                parts = (line[1] + line[2], line[0] + line[1], line[0], line[2])
                at = (tau * 2 + i) * MID_CH
                for g, part in enumerate(parts):
                    sums[a, g * OUT_CH : (g + 1) * OUT_CH, at : at + MID_CH] = part.astype(BF16)
            send = pltpu.make_async_copy(sums.at[a, :, lanes], out_ref.at[a, :, lanes], out_sems.at[tau * 2 + a])
            send.start()
            sends.append(send)
    for send in sends:
        send.wait()


def shifted(values, step, columns):
    if step == 1:
        return values
    rows = values.shape[0]
    x = iota(values.shape, 0) & (columns - 1)
    if step == 0:
        return jnp.where(x == 0, 0.0, pltpu.roll(values, 1, 0))
    return jnp.where(x == columns - 1, 0.0, pltpu.roll(values, rows - 1, 0))


def decode_kernel(
    incoming_ref,
    across_ref,
    code_ref,
    cached_ref,
    assign_hbm,
    counts_hbm,
    first_hbm,
    first_bias_hbm,
    gain_hbm,
    second_bias_hbm,
    features_ref,
    before_ref,
    after_ref,
    weight_ref,
    out_ref,
    latent_ref,
    next_ref,
    assign_ref,
    counts_ref,
    first_bias_ref,
    gain_ref,
    second_bias_ref,
    first_weight_ref,
    weave_ref,
    weight,
    second,
    padded,
    cells,
    window,
    received,
    halves,
    decoded,
    sems,
    out_sems,
):
    devices = lax.axis_size("seq")
    per_group = devices // REQS
    me = lax.axis_index("seq")
    place = (me + per_group // 2) & (devices - 1)
    position = place & (per_group - 1)
    copies = [
        pltpu.make_async_copy(features_ref, second.at[0:2, 1 : 1 + ROWS_DEV], sems.at[0]),
        pltpu.make_async_copy(first_hbm, first_weight_ref, sems.at[1]),
        pltpu.make_async_copy(weight_ref.at[0], weight.at[0], sems.at[2]),
        pltpu.make_async_copy(weight_ref.at[1], weight.at[1], sems.at[3]),
        pltpu.make_async_copy(assign_hbm, assign_ref, sems.at[4]),
        pltpu.make_async_copy(counts_hbm, counts_ref, sems.at[5]),
        pltpu.make_async_copy(first_bias_hbm, first_bias_ref, sems.at[6]),
        pltpu.make_async_copy(gain_hbm, gain_ref, sems.at[7]),
        pltpu.make_async_copy(second_bias_hbm, second_bias_ref, sems.at[8]),
    ]
    for copy in copies[4:] + copies[1:2] + copies[0:1] + copies[2:4]:
        copy.start()

    half = 2 * W
    at = iota((2 * half, 2 * half), 0)
    source_row = (at & (half - 1)) // W
    target = (at & (W - 1)) * 2 + at // half + source_row * half
    weave_ref[...] = (target == iota((2 * half, 2 * half), 1)).astype(F32).astype(BF16)

    per_peer = FX * ROWS_DEV // devices
    pairs = TILES * per_peer
    hot = jnp.concatenate(
        [(iota((FX, devices), 0) == across_ref[jk : jk + 1, :]).astype(F32).astype(BF16) for jk in range(pairs)], axis=1
    )
    wide = per_peer * LANES
    source = iota((LANES, wide), 1)
    expand = (iota((LANES, wide), 0) == source // LANES * LAT_CH + (source & (LAT_CH - 1))).astype(F32).astype(BF16)
    codes = code_ref[...].astype(I32) >> 8
    lane = iota((devices, LANES), 1) // LAT_CH + HALO
    received[...] = incoming_ref[...].astype(F32)
    for j in range(TILES):
        spread = dot(received[pl.ds(j, devices, stride=SLOTS), :].astype(BF16), expand)
        for k in range(per_peer):
            jk = j * per_peer + k
            part = jnp.where(lane == codes[:, jk : jk + 1], spread[:, k * LANES : (k + 1) * LANES], 0.0)
            cells[jk * devices : (jk + 1) * devices, :] = part.astype(BF16)
    arranged = dot(hot, cells[...])
    frames = jnp.concatenate([cached_ref[...].astype(F32), arranged], axis=0)
    for e in range(3):
        window[e] = shifted(frames, e, W).astype(BF16)

    for copy in copies[4:] + copies[1:2]:
        copy.wait()
    live = counts_ref[assign_ref[place // per_group]]
    margin = (WIN_ROWS - 3) * LAT_CH
    for a in range(3):
        for e in range(3):
            padded[a * 3 + e, 0:margin, :] = jnp.zeros((margin, MID_CH), BF16)
            padded[a * 3 + e, margin + 3 * LAT_CH :, :] = jnp.zeros((margin, MID_CH), BF16)
            for b in range(3):
                padded[a * 3 + e, margin + b * LAT_CH : margin + (b + 1) * LAT_CH, :] = first_weight_ref[a, b, e]

    taps = jnp.concatenate([window[e, a * W : a * W + FX, :] for a in range(3) for e in range(3)], axis=1)
    for r in range(MID_ROWS):
        start = (MID_ROWS - 1 - r) * LAT_CH
        kernel = jnp.concatenate([padded[ae, start : start + LANES, :] for ae in range(9)], axis=0)
        pre = dot(taps, kernel) + first_bias_ref[...][None, :]
        inverse = lax.rsqrt(jnp.mean(pre * pre, axis=1, keepdims=True) + 1e-06)
        linear = pre * inverse * gain_ref[...][None, :]
        active = linear / (1.0 + jnp.exp(-linear))
        if r == 0:
            active = jnp.where(position == 0, 0.0, active)
        if r == MID_ROWS - 1:
            active = jnp.where(position == per_group - 1, 0.0, active)
        for t in range(FMAX):
            second[2 + t, r] = active[t * W : (t + 1) * W, :].astype(BF16)
    for f in range(2):
        edge = before_ref[f, 0:W, :]
        second[f, 0] = jnp.where(position == 0, jnp.zeros_like(edge), edge)
        edge = after_ref[f, 0:W, :]
        second[f, MID_ROWS - 1] = jnp.where(position == per_group - 1, jnp.zeros_like(edge), edge)
    copies[0].wait()
    ahead = pltpu.make_async_copy(second.at[pl.ds(live, 2), 1 : 1 + ROWS_DEV], next_ref, sems.at[0])
    ahead.start()

    width = W * LAT_CH
    kept = window[1, pl.ds(pl.multiple_of(live * W, W), 2 * W), :]
    own = iota((2 * W, width), 1) // LAT_CH == (iota((2 * W, width), 0) & (W - 1))
    for y in range(ROWS_DEV):
        pick = iota((LANES, width), 0) == (iota((LANES, width), 1) & (LAT_CH - 1)) + (HALO + y) * LAT_CH
        flat = jnp.where(own, dot(kept, pick.astype(F32).astype(BF16)), 0.0)
        for f in range(2):
            latent_ref[f, y : y + 1, :] = jnp.sum(flat[f * W : (f + 1) * W], axis=0, keepdims=True).astype(BF16)

    pixels = ROWS_DEV * W
    diagonal = iota((OUT_CH, OUT_CH), 0) == iota((OUT_CH, OUT_CH), 1)
    bias = jnp.sum(jnp.where(diagonal, second_bias_ref[...][None, :], 0.0), axis=1, keepdims=True)
    column = iota((OUT_CH, pixels), 1) & (W - 1)
    def interleave(a):
        woven = dot(halves[a], weave_ref[...]).astype(BF16)
        for t in range(FMAX):
            for pair in range(ROWS_DEV // 2):
                start = (t * (ROWS_DEV // 2) + pair) * OUT_CH
                for y in range(2):
                    decoded[a, t, 2 * pair + y] = woven[start : start + OUT_CH, y * half : (y + 1) * half]
        pltpu.make_async_copy(decoded.at[a], out_ref.at[:, :, a], out_sems.at[a]).start()

    for a in range(2):
        copies[2 + a].wait()
        for t in range(FMAX):
            block = jnp.concatenate(
                [second[t + tau, a + i : a + i + ROWS_DEV].reshape(pixels, MID_CH) for tau in range(3) for i in range(2)],
                axis=1,
            )
            result = dot(weight[a], block, NT)
            left = pltpu.roll(result[2 * OUT_CH : 3 * OUT_CH], 1, 1)
            right = pltpu.roll(result[3 * OUT_CH : 4 * OUT_CH], pixels - 1, 1)
            even = result[0:OUT_CH] + jnp.where(column == 0, 0.0, left) + bias
            odd = result[OUT_CH : 2 * OUT_CH] + jnp.where(column == W - 1, 0.0, right) + bias
            even = jnp.where(t < live, even, 0.0).astype(BF16)
            odd = jnp.where(t < live, odd, 0.0).astype(BF16)
            for pair in range(ROWS_DEV // 2):
                lanes = slice(pair * half, (pair + 1) * half)
                start = (t * (ROWS_DEV // 2) + pair) * OUT_CH
                halves[a, start : start + OUT_CH, 0:half] = even[:, lanes]
                halves[a, start : start + OUT_CH, half : 2 * half] = odd[:, lanes]
        pl.when(live >= 0)(lambda a=a: interleave(a))
    for a in range(2):
        pltpu.make_async_copy(decoded.at[a], out_ref.at[:, :, a], out_sems.at[a]).wait()
    ahead.wait()


def in_vmem(array):
    return pltpu.with_memory_space_constraint(array, pltpu.VMEM)


def body(
    latents,
    layout,
    assign,
    counts,
    latent_cache,
    feature_cache,
    first_weight,
    first_bias,
    norm_gain,
    second_weight,
    second_bias,
):
    devices = lax.axis_size("seq")
    slots = layout.shape[1]
    per_peer = slots // devices
    pairs = TILES * per_peer
    up = [(i, (i + 1) % devices) for i in range(devices)]
    down = [(j, i) for i, j in up]

    edge = jax.ShapeDtypeStruct((2, W + 8, MID_CH), BF16)
    outgoing, last, first = pl.pallas_call(
        send_kernel,
        out_shape=(jax.ShapeDtypeStruct((devices * SLOTS, LANES), BF16), edge, edge),
        in_specs=[ANY] * 5,
        out_specs=(VMEM, VMEM, VMEM),
        scratch_shapes=[
            pltpu.VMEM((8, slots), I32),
            pltpu.VMEM(latents.shape, BF16),
            pltpu.VMEM(latent_cache.shape, BF16),
            pltpu.SMEM(assign.shape, I32),
            pltpu.VMEM((devices * SLOTS, LANES), F32),
            pltpu.SemaphoreType.DMA((6,)),
        ],
        name="send",
    )(layout, latents, assign, feature_cache, latent_cache)
    before = in_vmem(lax.ppermute(last, "seq", up))
    after = in_vmem(lax.ppermute(first, "seq", down))
    incoming = lax.all_to_all(
        outgoing.reshape(devices, SLOTS, LANES), "seq", split_axis=0, concat_axis=0, tiled=True
    ).reshape(devices * SLOTS, LANES)

    across, codes, cached = pl.pallas_call(
        table_kernel,
        out_shape=(
            pltpu.VMEM((LANES, devices), I32),
            pltpu.VMEM((devices, LANES), F32),
            pltpu.VMEM((2 * W, LANES), BF16),
        ),
        in_specs=[VMEM, SMEM, VMEM, VMEM, VMEM],
        out_specs=(VMEM, VMEM, VMEM),
        scratch_shapes=[pltpu.VMEM((WIN_ROWS * W, W * LAT_CH), BF16)],
        name="table",
    )(layout, assign, latent_cache, before, after)

    combined = pl.pallas_call(
        weight_kernel,
        out_shape=jax.ShapeDtypeStruct((2, 4 * OUT_CH, 6 * MID_CH), BF16),
        in_specs=[ANY],
        out_specs=ANY,
        scratch_shapes=[
            pltpu.VMEM((3, 3, 3, OUT_CH, MID_CH), BF16),
            pltpu.VMEM((2, 4 * OUT_CH, 6 * MID_CH), BF16),
            pltpu.SemaphoreType.DMA((3,)),
            pltpu.SemaphoreType.DMA((6,)),
        ],
        name="combine",
    )(jnp.swapaxes(second_weight, 3, 4))

    decoded, latent_next, feature_next = pl.pallas_call(
        decode_kernel,
        out_shape=(
            jax.ShapeDtypeStruct((FMAX, ROWS_DEV, 2, OUT_CH, 2 * W), BF16),
            jax.ShapeDtypeStruct((2, ROWS_DEV, W * LAT_CH), BF16),
            jax.ShapeDtypeStruct((2, ROWS_DEV, W, MID_CH), BF16),
        ),
        in_specs=[VMEM] * 4 + [ANY] * 7 + [VMEM] * 2 + [ANY],
        out_specs=(ANY, VMEM, ANY),
        scratch_shapes=[
            pltpu.SMEM(assign.shape, I32),
            pltpu.SMEM(counts.shape, I32),
            pltpu.VMEM(first_bias.shape, F32),
            pltpu.VMEM(norm_gain.shape, F32),
            pltpu.VMEM(second_bias.shape, F32),
            pltpu.VMEM(first_weight.shape, BF16),
            pltpu.VMEM((4 * W, 4 * W), BF16),
            pltpu.VMEM((2, 4 * OUT_CH, 6 * MID_CH), BF16),
            pltpu.VMEM((5, MID_ROWS, W, MID_CH), BF16),
            pltpu.VMEM((9, (2 * WIN_ROWS - 3) * LAT_CH, MID_CH), BF16),
            pltpu.VMEM((pairs * devices, LANES), BF16),
            pltpu.VMEM((3, 5 * W, LANES), BF16),
            pltpu.VMEM((devices * SLOTS, LANES), F32),
            pltpu.VMEM((2, FMAX * (ROWS_DEV // 2) * OUT_CH, 4 * W), BF16),
            pltpu.VMEM((2, FMAX, ROWS_DEV, OUT_CH, 2 * W), BF16),
            pltpu.SemaphoreType.DMA((9,)),
            pltpu.SemaphoreType.DMA((2,)),
        ],
        name="decode",
    )(
        in_vmem(incoming),
        in_vmem(across),
        in_vmem(codes),
        in_vmem(cached),
        assign,
        counts,
        first_weight,
        first_bias,
        norm_gain,
        second_bias,
        feature_cache,
        before,
        after,
        combined,
    )
    decoded = decoded.reshape(FMAX, 2 * ROWS_DEV, OUT_CH, 2 * W)
    return (jnp.swapaxes(decoded, 2, 3), latent_next, feature_next)


def solution(mesh):
    return jax.shard_map(
        body,
        mesh=mesh,
        in_specs=(
            P(None, ("rep", "seq")),
            P("rep", None),
            P("rep"),
            P("rep"),
            P(None, ("rep", "seq"), None),
            P(None, ("rep", "seq"), None, None),
            P(),
            P(),
            P(),
            P(),
            P(),
        ),
        out_specs=(
            P(None, ("rep", "seq"), None, None),
            P(None, ("rep", "seq"), None),
            P(None, ("rep", "seq"), None, None),
        ),
        check_vma=False,
    )
```
